32 devices in a mesh: tm: 4 (over y, x), space: 8 (over z, core).
Axes of the slice: x: 2, y: 2, z: 4, core: 2. Of those that a mesh axis runs over, the one named last changes fastest.
Arguments:
- initial_state: float32 [16, 256, 256], P('space'), may hold values from -6 to 6
- capacity: float32 [16, 256, 256], P('space'), may hold values from 0.5 to 2
- source: float32 [16, 256, 256], P('space'), may hold values from -6 to 6
- control: float32 [4, 16], P('tm'), may hold values from -2 to 2
- segment_index: int32 [16, 256], P('space'), may hold values from 0 to 15
Outputs:
- slice_ends: float32 [4, 16, 256, 256], P('tm', 'space')
The draws below stay inside these ranges and needn't reach their ends.
All inputs are finite; a program needn't handle non-finite values.
Results may differ from the reference program's by a relative error of at most 0.0001.
Values sent between devices are 32-bit elements; how exact they have to be, the bound alone decides.
A program may use at most 64 MiB of HBM per device.

```python
import math
import jax
import jax.numpy as jnp

NY = 256
NZ = 256
FINE = 1
SWEEPS = 6
CORRECTIONS = 2
SEGMENTS = 16
SLICES = 4
NX = 16


def touch_ends(result, key, smallest, high):
    longest = result.shape.index(max(result.shape))
    spots = []
    for shift in (0, 1):
        where = [jax.random.randint(jax.random.fold_in(key, axis), (), 0, length) for axis, length in enumerate(result.shape)]
        where[longest] = (where[longest] + shift) % result.shape[longest]
        spots.append(tuple(where))
    return result.at[spots[0]].set(smallest).at[spots[1]].set(high)


def block_levels(rng, dims, shards, least, top_value):
    gain, own = 1.0, jax.random.fold_in(rng, 6)
    for dim, blocks in shards:
        steps = jnp.exp(jax.random.uniform(jax.random.fold_in(own, dim), (blocks,), jnp.float32, least / len(shards), top_value / len(shards)))
        gain = gain * jnp.repeat(steps, dims[dim] // blocks).reshape([-1 if axis == dim else 1 for axis in range(len(dims))])
    return gain


def centred(stream_key, extent, spread, most, cuts=(), kind=jnp.bfloat16):
    result = spread * jax.random.normal(stream_key, extent, jnp.float32)
    if cuts:
        result = result * block_levels(stream_key, extent, cuts, -0.22, 0.18)
    return jnp.clip(result, -most, most).astype(kind)


def setup_inputs(seed: int = 0) -> dict:
    keys = jax.random.split(jax.random.key(seed), 6)
    return {
        "initial_state": centred(keys[0], (NX, NY, NZ), 1.0, 6.0, ((0, 8),), jnp.float32),
        "capacity": jnp.clip(jnp.exp(math.log(2.0) - 1.3862944 * jax.random.uniform(keys[1], (NX, NY, NZ), jnp.float32) ** block_levels(keys[1], (NX, NY, NZ), ((0, 8),), -0.2, 0.2)), 0.5, 2.0),
        "source": centred(keys[2], (NX, NY, NZ), 1.0, 6.0, ((0, 8),), jnp.float32),
        "control": jnp.clip(jax.random.uniform(keys[3], (SLICES, SEGMENTS), jnp.float32, -2.0, 2.0) * block_levels(keys[3], (SLICES, SEGMENTS), ((0, 4),), -0.4, 0.0), -2.0, 2.0),
        "segment_index": touch_ends(jax.random.randint(keys[4], (NX, NZ), 0, SEGMENTS), jax.random.fold_in(keys[4], 1), 0, SEGMENTS - 1).astype(jnp.int32),
    }


step_fine = 1.0
step_coarse = 0.08


def neighbours(extended):
    core = extended[1:-1]
    total = extended[2:] + extended[:-2]
    wide = jnp.pad(core, ((0, 0), (1, 1), (0, 0)))
    total = total + wide[:, 2:] + wide[:, :-2]
    deeper = jnp.pad(core, ((0, 0), (0, 0), (1, 1)))
    return total + deeper[:, :, 2:] + deeper[:, :, :-2]


def jacobi_sweep(extended, previous, capacity, forcing, divisor):
    return (capacity * previous + step_fine * forcing + step_fine * neighbours(extended)) / divisor


def coarse_step(extended, scale, forcing):
    core = extended[1:-1]
    return core + scale * (neighbours(extended) - 6.0 * core + forcing)


def pad_planes(field):
    return jnp.pad(field, ((1, 1), (0, 0), (0, 0)))


def boundary_forcing(source, segment_index, control_row):
    matches = segment_index[:, None, :] == jnp.arange(SEGMENTS, dtype=jnp.int32)[None, :, None]
    values = jnp.sum(jnp.where(matches, control_row[None, :, None], jnp.zeros((), source.dtype)), axis=1)
    return source + jnp.pad(values[:, None, :], ((0, 0), (0, source.shape[1] - 1), (0, 0)))


def reference(initial_state, capacity, source, control, segment_index):
    divisor = capacity + 6.0 * step_fine
    scale = step_coarse / capacity
    forcings = [boundary_forcing(source, segment_index, control[slice_index]) for slice_index in range(SLICES)]

    def fine_solve(state, forcing):
        for fine_index in range(FINE):
            iterate = state
            for sweep_index in range(SWEEPS):
                iterate = jacobi_sweep(pad_planes(iterate), state, capacity, forcing, divisor)
            state = iterate
        return state

    starts = [initial_state]
    coarse_values = []
    for slice_index in range(SLICES):
        value = coarse_step(pad_planes(starts[slice_index]), scale, forcings[slice_index])
        coarse_values.append(value)
        if slice_index + 1 < SLICES:
            starts.append(value)
    ends = []
    for correction_index in range(CORRECTIONS):
        deltas = [fine_solve(starts[n], forcings[n]) - coarse_values[n] for n in range(SLICES)]
        new_starts = [initial_state]
        new_values = []
        ends = []
        for slice_index in range(SLICES):
            value = coarse_step(pad_planes(new_starts[slice_index]), scale, forcings[slice_index])
            new_values.append(value)
            end_state = value + deltas[slice_index]
            ends.append(end_state)
            if slice_index + 1 < SLICES:
                new_starts.append(end_state)
        starts = new_starts
        coarse_values = new_values
    return jnp.stack(ends)
```

```python
import functools

import jax
import jax.numpy as jnp
from jax import lax
from jax.experimental import pallas as pl
from jax.experimental.pallas import tpu as pltpu
from jax.sharding import PartitionSpec as P

SWEEPS = 6
CORRECTIONS = 2
step_fine = 1.0
step_coarse = 0.08


def make_plan(slices):
    last = CORRECTIONS
    solves = [
        (k, n)
        for k in range(last)
        for n in range(k, slices)
        if k == last - 1 or n + 1 < slices or n == k
    ]
    slots, sent = {}, set()
    for k, n in solves:
        for j in range(SWEEPS):
            slots[(k, n, j)] = len(slots)
            sent.add((k, n, j))

    def state(k, n):
        k = min(k, n)
        key = (k, n, 0)
        if key not in slots:
            slots[key] = len(slots)
        return key

    ends = [state(last, n + 1) for n in range(slices)]
    rounds = {}
    top_coarse = max(n for k, n in solves if k == 0)
    for n in range(top_coarse):
        rounds.setdefault(n + 1, []).append(("coarse", n, state(0, n), state(0, n + 1)))
    for k, n in sorted(solves, key=lambda item: (-item[0], item[1])):
        begin = SWEEPS * k + n - k
        for j in range(1, SWEEPS + 1):
            target = (k, n, j) if j < SWEEPS else state(k + 1, n + 1)
            pair = None
            if j == SWEEPS and k < n:
                pair = (state(k + 1, n), state(k, n))
                sent.add(pair[0])
                sent.add(pair[1])
            rounds.setdefault(begin + j, []).append(("sweep", n, (k, n, j - 1), target, j, pair))
    return slots, sent, [rounds[r] for r in sorted(rounds)], ends


def kernel(plan, size, state_hbm, cap_hbm, src_hbm, ctrl_ref, seg_ref, out_hbm,
           field, forcing, base, inv, scale, source, ctrl_all,
           send_sem, recv_sem, in_sem, ctrl_send, ctrl_recv, out_send, out_recv, own_sem):
    slots, sent, rounds, ends = plan
    planes, window, own_rows, reach, rows, cols, slices, count = size
    t = lax.axis_index("tm")
    s = lax.axis_index("space")
    low_there, high_there = s > 0, s < count - 1
    first_row = pl.multiple_of(jnp.clip(t * own_rows - reach, 0, rows - window), 8)
    own_at = pl.multiple_of(t * own_rows - first_row, 8)
    inner = pl.ds(1, planes)
    first = slots[(0, 0, 0)]

    loads = []
    for index, (ref, target) in enumerate(
        ((state_hbm, field.at[first, inner]), (cap_hbm, inv), (src_hbm, source))
    ):
        loads.append(pltpu.make_async_copy(ref.at[:, pl.ds(first_row, window), :], target, in_sem.at[index]))
        loads[-1].start()

    @pl.when(jnp.logical_not(low_there))
    def _():
        for key in sorted(sent):
            field[slots[key], 0] = jnp.zeros((window, cols), jnp.float32)

    @pl.when(jnp.logical_not(high_there))
    def _():
        for key in sorted(sent):
            field[slots[key], planes + 1] = jnp.zeros((window, cols), jnp.float32)

    barrier = pltpu.get_barrier_semaphore()

    @pl.when(low_there)
    def _():
        pl.semaphore_signal(barrier, inc=1, device_id={"space": s - 1})

    @pl.when(high_there)
    def _():
        pl.semaphore_signal(barrier, inc=1, device_id={"space": s + 1})

    for hop in range(1, slices):
        pl.semaphore_signal(barrier, inc=1, device_id={"tm": lax.rem(t + hop, slices)})
    pl.semaphore_wait(barrier, slices - 1 + jnp.minimum(s, 1) + jnp.minimum(count - 1 - s, 1))

    def halo(key, side):
        slot = slots[key]
        if side == 0:
            source_plane, target_plane, other = 1, planes + 1, s - 1
        else:
            source_plane, target_plane, other = planes, 0, s + 1
        return pltpu.make_async_remote_copy(
            src_ref=field.at[slot, source_plane],
            dst_ref=field.at[slot, target_plane],
            send_sem=send_sem.at[slot, side],
            recv_sem=recv_sem.at[slot, side],
            device_id={"space": other},
        )

    def send(key):
        if key in sent:
            for side, there in ((0, low_there), (1, high_there)):

                @pl.when(there)
                def _():
                    halo(key, side).start()

    arrived = set()

    def arrive(key):
        if key in arrived:
            return
        arrived.add(key)
        for side, there in ((0, high_there), (1, low_there)):

            @pl.when(there)
            def _():
                halo(key, side).wait_recv()

    loads[0].wait()
    send((0, 0, 0))

    ctrl_copies = []
    for hop in range(1, slices):
        ctrl_copies.append(pltpu.make_async_remote_copy(
            src_ref=ctrl_ref,
            dst_ref=ctrl_all.at[hop],
            send_sem=ctrl_send.at[hop],
            recv_sem=ctrl_recv.at[hop],
            device_id={"tm": lax.rem(t + hop, slices)},
        ))
        ctrl_copies[-1].start()
    own_ctrl = pltpu.make_async_copy(ctrl_ref, ctrl_all.at[0], own_sem.at[0])
    own_ctrl.start()

    loads[1].wait()
    capacity = inv[...]
    scale[...] = step_coarse / capacity
    reciprocal = 1.0 / (capacity + 6.0 * step_fine)
    inv[...] = reciprocal
    loads[2].wait()
    own_ctrl.wait()
    for copy in ctrl_copies:
        copy.wait_recv()

    segment = seg_ref[...]
    segments = ctrl_ref.shape[1]
    row_id = lax.broadcasted_iota(jnp.int32, (planes, window, cols), 1) + first_row
    for n in range(slices):
        row = jnp.zeros((1, segments), jnp.float32)
        for hop in range(slices):
            row = jnp.where(lax.rem(t - n + slices, slices) == hop, ctrl_all[hop], row)
        values = jnp.zeros((planes, cols), jnp.float32)
        for k in range(segments):
            values = jnp.where(segment == k, row[:, k:k + 1], values)
        forcing[n] = source[...] + jnp.where(row_id == 0, values[:, None, :], 0.0)

    step = window // 2 if window % 16 == 0 else window
    lane = lax.broadcasted_iota(jnp.int32, (step, cols), 1)
    line = lax.broadcasted_iota(jnp.int32, (step, cols), 0)
    pieces = [(p, r) for p in range(planes) for r in range(0, window, step)]

    def neighbours(read, p, r):
        core = read(p + 1, r)
        if r > 0:
            above = read(p + 1, r - 1)
        else:
            above = jnp.where(line == 0, 0.0, pltpu.roll(core, 1, 0))
        if r + step < window:
            below = read(p + 1, r + 1)
        else:
            below = jnp.where(line == step - 1, 0.0, pltpu.roll(core, step - 1, 0))
        left = jnp.where(lane == 0, 0.0, pltpu.roll(core, 1, 1))
        right = jnp.where(lane == cols - 1, 0.0, pltpu.roll(core, cols - 1, 1))
        return core, read(p, r) + read(p + 2, r) + above + below + left + right

    def reader(key):
        return lambda p, r: field[slots[key], p, pl.ds(r, step)]

    def difference(new, old):
        return lambda p, r: field[slots[new], p, pl.ds(r, step)] - field[slots[old], p, pl.ds(r, step)]

    def piece(ref, p, r):
        return ref[p, pl.ds(r, step)]

    def result(n, end):
        def remote(target, source_slice):
            return pltpu.make_async_remote_copy(
                src_ref=field.at[slots[end], inner, pl.ds(own_at, own_rows)],
                dst_ref=out_hbm.at[0, :, pl.ds(pl.multiple_of(source_slice * own_rows, 8), own_rows)],
                send_sem=out_send.at[target],
                recv_sem=out_recv.at[source_slice],
                device_id={"tm": target},
            )
        return remote

    def own_copy(n):
        return pltpu.make_async_copy(
            field.at[slots[ends[n]], inner, pl.ds(own_at, own_rows)],
            out_hbm.at[0, :, pl.ds(n * own_rows, own_rows)],
            own_sem.at[1],
        )

    def emit(key):
        for n, end in enumerate(ends):
            if end == key:

                @pl.when(t != n)
                def _():
                    result(n, end)(n, t).start()

                @pl.when(t == n)
                def _():
                    own_copy(n).start()

    for tasks in rounds:
        for task in tasks:
            if task[0] == "coarse":
                _, n, source_key, target = task
                arrive(source_key)
                for p, r in pieces:
                    core, around = neighbours(reader(source_key), p, r)
                    field[slots[target], p + 1, pl.ds(r, step)] = core + piece(scale, p, r) * (
                        around - 6.0 * core + piece(forcing.at[n], p, r)
                    )
            else:
                _, n, source_key, target, j, pair = task
                held = source_key[0] % 2 * slices + n
                arrive(source_key)
                if pair is not None:
                    arrive(pair[0])
                    arrive(pair[1])
                for p, r in pieces:
                    core, around = neighbours(reader(source_key), p, r)
                    gain = piece(inv, p, r)
                    if j == 1:
                        constant = core - gain * (6.0 * step_fine * core - step_fine * piece(forcing.at[n], p, r))
                        base[held, p, pl.ds(r, step)] = constant
                    else:
                        constant = piece(base.at[held], p, r)
                    value = constant + step_fine * gain * around
                    if pair is not None:
                        change, spread = neighbours(difference(*pair), p, r)
                        value = value + change + piece(scale, p, r) * (spread - 6.0 * change)
                    field[slots[target], p + 1, pl.ds(r, step)] = value
            send(target)
            emit(target)

    for key in sorted(sent):
        arrive(key)
        for side, there in ((0, low_there), (1, high_there)):

            @pl.when(there)
            def _():
                halo(key, side).wait_send()

    for copy in ctrl_copies:
        copy.wait_send()
    for n in range(slices):

        @pl.when(t != n)
        def _():
            result(n, ends[n])(n, t).wait_send()
            result(n, ends[n])(t, n).wait_recv()

        @pl.when(t == n)
        def _():
            own_copy(n).wait()


def solution(mesh):
    slices, count = mesh.shape["tm"], mesh.shape["space"]
    plan = make_plan(slices)

    def on_device(initial_state, capacity, source, control, segment_index):
        planes, rows, cols = initial_state.shape
        own_rows = rows // slices
        reach = -(-(CORRECTIONS * SWEEPS + slices - CORRECTIONS) // 8) * 8
        window = min(rows, own_rows + 2 * reach)
        fields = len(plan[0])
        size = (planes, window, own_rows, reach, rows, cols, slices, count)
        block = (planes, window, cols)
        dma = pltpu.SemaphoreType.DMA
        return pl.pallas_call(
            functools.partial(kernel, plan, size),
            out_shape=jax.ShapeDtypeStruct((1, planes, rows, cols), jnp.float32),
            in_specs=[pl.BlockSpec(memory_space=pl.ANY)] * 3 + [pl.BlockSpec(memory_space=pltpu.VMEM)] * 2,
            out_specs=pl.BlockSpec(memory_space=pl.ANY),
            scratch_shapes=[
                pltpu.VMEM((fields, planes + 2, window, cols), jnp.float32),
                pltpu.VMEM((slices,) + block, jnp.float32),
                pltpu.VMEM((2 * slices,) + block, jnp.float32),
                pltpu.VMEM(block, jnp.float32),
                pltpu.VMEM(block, jnp.float32),
                pltpu.VMEM(block, jnp.float32),
                pltpu.VMEM((slices,) + control.shape, jnp.float32),
                dma((fields, 2)),
                dma((fields, 2)),
                dma((3,)),
                dma((slices,)),
                dma((slices,)),
                dma((slices,)),
                dma((slices,)),
                dma((2,)),
            ],
            compiler_params=pltpu.CompilerParams(
                collective_id=0, has_side_effects=True, vmem_limit_bytes=67043328 - 1048576
            ),
        )(initial_state, capacity, source, control, segment_index)

    return jax.shard_map(
        on_device,
        mesh=mesh,
        in_specs=(
            P("space", None, None),
            P("space", None, None),
            P("space", None, None),
            P("tm", None),
            P("space", None),
        ),
        out_specs=P("tm", "space", None, None),
        check_vma=False,
    )
```

```python
import functools

import jax
import jax.numpy as jnp
from jax import lax
from jax.experimental import pallas as pl
from jax.experimental.pallas import tpu as pltpu
from jax.sharding import PartitionSpec as P

SWEEPS = 6
CORRECTIONS = 2
step_fine = 1.0
step_coarse = 0.08


def make_plan(slices):
    last = CORRECTIONS
    solves = [
        (k, n)
        for k in range(last)
        for n in range(k, slices)
        if k == last - 1 or n + 1 < slices or n == k
    ]
    slots, sent = {}, set()
    for k, n in solves:
        for j in range(SWEEPS):
            slots[(k, n, j)] = len(slots)
            sent.add((k, n, j))

    def state(k, n):
        k = min(k, n)
        key = (k, n, 0)
        if key not in slots:
            slots[key] = len(slots)
        return key

    ends = [state(last, n + 1) for n in range(slices)]
    rounds = {}
    top_coarse = max(n for k, n in solves if k == 0)
    for n in range(top_coarse):
        rounds.setdefault(n + 1, []).append(("coarse", n, state(0, n), state(0, n + 1)))
    for k, n in sorted(solves, key=lambda item: (-item[0], item[1])):
        begin = SWEEPS * k + n - k
        for j in range(1, SWEEPS + 1):
            target = (k, n, j) if j < SWEEPS else state(k + 1, n + 1)
            pair = None
            if j == SWEEPS and k < n:
                pair = (state(k + 1, n), state(k, n))
                sent.add(pair[0])
                sent.add(pair[1])
            rounds.setdefault(begin + j, []).append(("sweep", n, (k, n, j - 1), target, j, pair))
    return slots, sent, [rounds[r] for r in sorted(rounds)], ends


def row_order(groups):
    if groups & (groups - 1):
        return list(range(groups))
    return [i ^ (i >> 1) for i in range(groups)]


def kernel(plan, size, state_hbm, cap_hbm, src_hbm, ctrl_ref, seg_ref, out_hbm,
           field, edge, forcing, base, inv, scale, source, ctrl_all,
           send_sem, recv_sem, in_sem, ctrl_send, ctrl_recv, out_send, out_recv, own_sem,
           edge_send, edge_recv):
    slots, sent, rounds, ends = plan
    planes, own_rows, rows, cols, slices, count = size
    t = lax.axis_index("tm")
    s = lax.axis_index("space")
    low_there, high_there = s > 0, s < count - 1
    order = row_order(slices)
    block, before, after = 0, 0, 0
    for place, group in enumerate(order):
        block = jnp.where(t == group, place, block)
        before = jnp.where(t == group, order[max(place - 1, 0)], before)
        after = jnp.where(t == group, order[min(place + 1, slices - 1)], after)
    before_there, after_there = block > 0, block < slices - 1
    first_row = pl.multiple_of(block * own_rows, 8)
    inner = pl.ds(1, planes)
    first = slots[(0, 0, 0)]

    loads = []
    for index, (ref, target) in enumerate(
        ((state_hbm, field.at[first, inner]), (cap_hbm, inv), (src_hbm, source))
    ):
        loads.append(pltpu.make_async_copy(ref.at[:, pl.ds(first_row, own_rows), :], target, in_sem.at[index]))
        loads[-1].start()

    @pl.when(jnp.logical_not(low_there))
    def _():
        for key in sorted(sent):
            field[slots[key], 0] = jnp.zeros((own_rows, cols), jnp.float32)

    @pl.when(jnp.logical_not(high_there))
    def _():
        for key in sorted(sent):
            field[slots[key], planes + 1] = jnp.zeros((own_rows, cols), jnp.float32)

    for side, there in ((0, before_there), (1, after_there)):

        @pl.when(jnp.logical_not(there))
        def _():
            for key in sorted(sent):
                edge[slots[key], side] = jnp.zeros((planes, 8, cols), jnp.float32)

    barrier = pltpu.get_barrier_semaphore()

    @pl.when(low_there)
    def _():
        pl.semaphore_signal(barrier, inc=1, device_id={"space": s - 1})

    @pl.when(high_there)
    def _():
        pl.semaphore_signal(barrier, inc=1, device_id={"space": s + 1})

    for hop in range(1, slices):
        pl.semaphore_signal(barrier, inc=1, device_id={"tm": lax.rem(t + hop, slices)})
    pl.semaphore_wait(barrier, slices - 1 + jnp.minimum(s, 1) + jnp.minimum(count - 1 - s, 1))

    def halo(key, side):
        slot = slots[key]
        if side == 0:
            source_plane, target_plane, other = 1, planes + 1, s - 1
        else:
            source_plane, target_plane, other = planes, 0, s + 1
        return pltpu.make_async_remote_copy(
            src_ref=field.at[slot, source_plane],
            dst_ref=field.at[slot, target_plane],
            send_sem=send_sem.at[slot, side],
            recv_sem=recv_sem.at[slot, side],
            device_id={"space": other},
        )

    def rim(key, side):
        slot = slots[key]
        return pltpu.make_async_remote_copy(
            src_ref=field.at[slot, inner, pl.ds(0 if side == 0 else own_rows - 8, 8)],
            dst_ref=edge.at[slot, 1 - side],
            send_sem=edge_send.at[slot, side],
            recv_sem=edge_recv.at[slot, side],
            device_id={"tm": before if side == 0 else after},
        )

    def send(key):
        if key in sent:
            for side, there in ((0, low_there), (1, high_there)):

                @pl.when(there)
                def _():
                    halo(key, side).start()

            for side, there in ((0, before_there), (1, after_there)):

                @pl.when(there)
                def _():
                    rim(key, side).start()

    arrived = set()

    def arrive(key):
        if key in arrived:
            return
        arrived.add(key)
        for side, there in ((0, high_there), (1, low_there)):

            @pl.when(there)
            def _():
                halo(key, side).wait_recv()

        for side, there in ((0, after_there), (1, before_there)):

            @pl.when(there)
            def _():
                rim(key, side).wait_recv()

    loads[0].wait()
    send((0, 0, 0))

    ctrl_copies = []
    for hop in range(1, slices):
        ctrl_copies.append(pltpu.make_async_remote_copy(
            src_ref=ctrl_ref,
            dst_ref=ctrl_all.at[hop],
            send_sem=ctrl_send.at[hop],
            recv_sem=ctrl_recv.at[hop],
            device_id={"tm": lax.rem(t + hop, slices)},
        ))
        ctrl_copies[-1].start()
    own_ctrl = pltpu.make_async_copy(ctrl_ref, ctrl_all.at[0], own_sem.at[0])
    own_ctrl.start()

    loads[1].wait()
    capacity = inv[...]
    scale[...] = step_coarse / capacity
    reciprocal = 1.0 / (capacity + 6.0 * step_fine)
    inv[...] = reciprocal
    loads[2].wait()
    own_ctrl.wait()
    for copy in ctrl_copies:
        copy.wait_recv()

    segment = seg_ref[...]
    segments = ctrl_ref.shape[1]
    row_id = lax.broadcasted_iota(jnp.int32, (planes, own_rows, cols), 1) + first_row
    for n in range(slices):
        row = jnp.zeros((1, segments), jnp.float32)
        for hop in range(slices):
            row = jnp.where(lax.rem(t - n + slices, slices) == hop, ctrl_all[hop], row)
        values = jnp.zeros((planes, cols), jnp.float32)
        for k in range(segments):
            values = jnp.where(segment == k, row[:, k:k + 1], values)
        forcing[n] = source[...] + jnp.where(row_id == 0, values[:, None, :], 0.0)

    step = own_rows // 2 if own_rows % 16 == 0 else own_rows
    lane = lax.broadcasted_iota(jnp.int32, (step, cols), 1)
    line = lax.broadcasted_iota(jnp.int32, (step, cols), 0)
    pieces = [(p, r) for p in range(planes) for r in range(0, own_rows, step)]

    def neighbours(read, p, r):
        core = read(p + 1, r)
        if r > 0:
            above = read(p + 1, r - 1)
        else:
            above = jnp.where(line == 0, read(p, None, 0), pltpu.roll(core, 1, 0))
        if r + step < own_rows:
            below = read(p + 1, r + 1)
        else:
            below = jnp.where(line == step - 1, read(p, None, 1), pltpu.roll(core, step - 1, 0))
        left = jnp.where(lane == 0, 0.0, pltpu.roll(core, 1, 1))
        right = jnp.where(lane == cols - 1, 0.0, pltpu.roll(core, cols - 1, 1))
        return core, read(p, r) + read(p + 2, r) + above + below + left + right

    def reader(key):
        slot = slots[key]

        def read(p, r, side=0):
            if r is None:
                return edge[slot, side, p, 7:8] if side == 0 else edge[slot, side, p, 0:1]
            return field[slot, p, pl.ds(r, step)]

        return read

    def difference(new, old):
        return lambda *place: reader(new)(*place) - reader(old)(*place)

    def piece(ref, p, r):
        return ref[p, pl.ds(r, step)]

    def result(n, end):
        def remote(target, source_slice):
            return pltpu.make_async_remote_copy(
                src_ref=field.at[slots[end], inner],
                dst_ref=out_hbm.at[0, :, pl.ds(first_row, own_rows)],
                send_sem=out_send.at[target],
                recv_sem=out_recv.at[source_slice],
                device_id={"tm": target},
            )
        return remote

    def own_copy(n):
        return pltpu.make_async_copy(
            field.at[slots[ends[n]], inner],
            out_hbm.at[0, :, pl.ds(first_row, own_rows)],
            own_sem.at[1],
        )

    def emit(key):
        for n, end in enumerate(ends):
            if end == key:

                @pl.when(t != n)
                def _():
                    result(n, end)(n, t).start()

                @pl.when(t == n)
                def _():
                    own_copy(n).start()

    for tasks in rounds:
        for task in tasks:
            if task[0] == "coarse":
                _, n, source_key, target = task
                arrive(source_key)
                for p, r in pieces:
                    core, around = neighbours(reader(source_key), p, r)
                    field[slots[target], p + 1, pl.ds(r, step)] = core + piece(scale, p, r) * (
                        around - 6.0 * core + piece(forcing.at[n], p, r)
                    )
            else:
                _, n, source_key, target, j, pair = task
                held = source_key[0] % 2 * slices + n
                arrive(source_key)
                if pair is not None:
                    arrive(pair[0])
                    arrive(pair[1])
                for p, r in pieces:
                    core, around = neighbours(reader(source_key), p, r)
                    gain = piece(inv, p, r)
                    if j == 1:
                        constant = core - gain * (6.0 * step_fine * core - step_fine * piece(forcing.at[n], p, r))
                        base[held, p, pl.ds(r, step)] = constant
                    else:
                        constant = piece(base.at[held], p, r)
                    value = constant + step_fine * gain * around
                    if pair is not None:
                        change, spread = neighbours(difference(*pair), p, r)
                        value = value + change + piece(scale, p, r) * (spread - 6.0 * change)
                    field[slots[target], p + 1, pl.ds(r, step)] = value
            send(target)
            emit(target)

    for key in sorted(sent):
        arrive(key)
        for side, there in ((0, low_there), (1, high_there)):

            @pl.when(there)
            def _():
                halo(key, side).wait_send()

        for side, there in ((0, before_there), (1, after_there)):

            @pl.when(there)
            def _():
                rim(key, side).wait_send()

    for copy in ctrl_copies:
        copy.wait_send()
    for n in range(slices):

        @pl.when(t != n)
        def _():
            result(n, ends[n])(n, t).wait_send()
            result(n, ends[n])(t, n).wait_recv()

        @pl.when(t == n)
        def _():
            own_copy(n).wait()


def solution(mesh):
    slices, count = mesh.shape["tm"], mesh.shape["space"]
    plan = make_plan(slices)

    def on_device(initial_state, capacity, source, control, segment_index):
        planes, rows, cols = initial_state.shape
        own_rows = rows // slices
        fields = len(plan[0])
        size = (planes, own_rows, rows, cols, slices, count)
        block = (planes, own_rows, cols)
        held = fields * ((planes + 2) * own_rows + 16 * planes) + (3 * slices + 3) * planes * own_rows
        dma = pltpu.SemaphoreType.DMA
        return pl.pallas_call(
            functools.partial(kernel, plan, size),
            out_shape=jax.ShapeDtypeStruct((1, planes, rows, cols), jnp.float32),
            in_specs=[pl.BlockSpec(memory_space=pl.ANY)] * 3 + [pl.BlockSpec(memory_space=pltpu.VMEM)] * 2,
            out_specs=pl.BlockSpec(memory_space=pl.ANY),
            scratch_shapes=[
                pltpu.VMEM((fields, planes + 2, own_rows, cols), jnp.float32),
                pltpu.VMEM((fields, 2, planes, 8, cols), jnp.float32),
                pltpu.VMEM((slices,) + block, jnp.float32),
                pltpu.VMEM((2 * slices,) + block, jnp.float32),
                pltpu.VMEM(block, jnp.float32),
                pltpu.VMEM(block, jnp.float32),
                pltpu.VMEM(block, jnp.float32),
                pltpu.VMEM((slices,) + control.shape, jnp.float32),
                dma((fields, 2)),
                dma((fields, 2)),
                dma((3,)),
                dma((slices,)),
                dma((slices,)),
                dma((slices,)),
                dma((slices,)),
                dma((2,)),
                dma((fields, 2)),
                dma((fields, 2)),
            ],
            compiler_params=pltpu.CompilerParams(
                collective_id=0, has_side_effects=True, vmem_limit_bytes=4 * cols * held + 3 * 1048576
            ),
        )(initial_state, capacity, source, control, segment_index)

    return jax.shard_map(
        on_device,
        mesh=mesh,
        in_specs=(
            P("space", None, None),
            P("space", None, None),
            P("space", None, None),
            P("tm", None),
            P("space", None),
        ),
        out_specs=P("tm", "space", None, None),
        check_vma=False,
    )
```

```python
import functools

import jax
import jax.numpy as jnp
from jax import lax
from jax.experimental import pallas as pl
from jax.experimental.pallas import tpu as pltpu
from jax.sharding import PartitionSpec as P

SWEEPS = 6
CORRECTIONS = 2
step_fine = 1.0
step_coarse = 0.08


def make_plan(slices):
    last = CORRECTIONS
    solves = [
        (k, n)
        for k in range(last)
        for n in range(k, slices)
        if k == last - 1 or n + 1 < slices or n == k
    ]
    slots, sent = {}, set()
    for k, n in solves:
        for j in range(SWEEPS):
            slots[(k, n, j)] = len(slots)
            sent.add((k, n, j))

    def state(k, n):
        k = min(k, n)
        key = (k, n, 0)
        if key not in slots:
            slots[key] = len(slots)
        return key

    ends = [state(last, n + 1) for n in range(slices)]
    rounds = {}
    top_coarse = max(n for k, n in solves if k == 0)
    for n in range(top_coarse):
        rounds.setdefault(n + 1, []).append(("coarse", n, state(0, n), state(0, n + 1)))
    for k, n in sorted(solves, key=lambda item: (-item[0], item[1])):
        begin = SWEEPS * k + n - k
        for j in range(1, SWEEPS + 1):
            target = (k, n, j) if j < SWEEPS else state(k + 1, n + 1)
            pair = None
            if j == SWEEPS and k < n:
                pair = (state(k + 1, n), state(k, n))
                sent.add(pair[0])
                sent.add(pair[1])
            rounds.setdefault(begin + j, []).append(("sweep", n, (k, n, j - 1), target, j, pair))
    return slots, sent, [rounds[r] for r in sorted(rounds)], ends


def kernel(plan, size, state_hbm, cap_hbm, src_hbm, ctrl_ref, seg_ref, out_hbm,
           field, forcing, base, inv, scale, source, ctrl_all,
           send_sem, recv_sem, in_sem, ctrl_send, ctrl_recv, out_send, out_recv, own_sem):
    slots, sent, rounds, ends = plan
    planes, window, own_rows, reach, rows, cols, slices, count = size
    t = lax.axis_index("tm")
    s = lax.axis_index("space")
    low_there, high_there = s > 0, s < count - 1
    first_row = pl.multiple_of(jnp.clip(t * own_rows - reach, 0, rows - window), 8)
    own_at = pl.multiple_of(t * own_rows - first_row, 8)
    inner = pl.ds(1, planes)
    first = slots[(0, 0, 0)]

    loads = []
    for index, (ref, target) in enumerate(
        ((state_hbm, field.at[first, inner]), (cap_hbm, inv), (src_hbm, source))
    ):
        loads.append(pltpu.make_async_copy(ref.at[:, pl.ds(first_row, window), :], target, in_sem.at[index]))
        loads[-1].start()

    @pl.when(jnp.logical_not(low_there))
    def _():
        for key in sorted(sent):
            field[slots[key], 0] = jnp.zeros((window, cols), jnp.float32)

    @pl.when(jnp.logical_not(high_there))
    def _():
        for key in sorted(sent):
            field[slots[key], planes + 1] = jnp.zeros((window, cols), jnp.float32)

    barrier = pltpu.get_barrier_semaphore()

    @pl.when(low_there)
    def _():
        pl.semaphore_signal(barrier, inc=1, device_id={"space": s - 1})

    @pl.when(high_there)
    def _():
        pl.semaphore_signal(barrier, inc=1, device_id={"space": s + 1})

    for hop in range(1, slices):
        pl.semaphore_signal(barrier, inc=1, device_id={"tm": lax.rem(t + hop, slices)})
    pl.semaphore_wait(barrier, slices - 1 + jnp.minimum(s, 1) + jnp.minimum(count - 1 - s, 1))

    def halo(key, side):
        slot = slots[key]
        if side == 0:
            source_plane, target_plane, other = 1, planes + 1, s - 1
        else:
            source_plane, target_plane, other = planes, 0, s + 1
        k, n, j = key
        left = CORRECTIONS * (SWEEPS - 1) + slices - (k * (SWEEPS - 1) + n + j)
        near = min(-(-left // 8) * 8, reach)
        height = min(window, own_rows + 2 * near)
        at = jnp.clip(t * own_rows - near, 0, rows - height) - first_row
        needed = pl.ds(pl.multiple_of(at, 8), height)
        return pltpu.make_async_remote_copy(
            src_ref=field.at[slot, source_plane, needed],
            dst_ref=field.at[slot, target_plane, needed],
            send_sem=send_sem.at[slot, side],
            recv_sem=recv_sem.at[slot, side],
            device_id={"space": other},
        )

    odd = lax.rem(s, 2)

    def send(key, parts=(0, 1)):
        if key in sent:
            for part in parts:
                for side, there in ((0, low_there), (1, high_there)):

                    @pl.when(jnp.logical_and(there, odd == (side + part) % 2))
                    def _():
                        halo(key, side).start()

    arrived = set()

    def arrive(key):
        if key in arrived:
            return
        arrived.add(key)
        for side, there in ((0, high_there), (1, low_there)):

            @pl.when(there)
            def _():
                halo(key, side).wait_recv()

    loads[0].wait()
    send((0, 0, 0))

    ctrl_copies = []
    for hop in range(1, slices):
        ctrl_copies.append(pltpu.make_async_remote_copy(
            src_ref=ctrl_ref,
            dst_ref=ctrl_all.at[hop],
            send_sem=ctrl_send.at[hop],
            recv_sem=ctrl_recv.at[hop],
            device_id={"tm": lax.rem(t + hop, slices)},
        ))
        ctrl_copies[-1].start()
    own_ctrl = pltpu.make_async_copy(ctrl_ref, ctrl_all.at[0], own_sem.at[0])
    own_ctrl.start()

    loads[1].wait()
    capacity = inv[...]
    scale[...] = step_coarse / capacity
    reciprocal = 1.0 / (capacity + 6.0 * step_fine)
    inv[...] = reciprocal
    loads[2].wait()
    own_ctrl.wait()
    for copy in ctrl_copies:
        copy.wait_recv()

    segment = seg_ref[...]
    segments = ctrl_ref.shape[1]
    row_id = lax.broadcasted_iota(jnp.int32, (planes, window, cols), 1) + first_row
    for n in range(slices):
        row = jnp.zeros((1, segments), jnp.float32)
        for hop in range(slices):
            row = jnp.where(lax.rem(t - n + slices, slices) == hop, ctrl_all[hop], row)
        values = jnp.zeros((planes, cols), jnp.float32)
        for k in range(segments):
            values = jnp.where(segment == k, row[:, k:k + 1], values)
        forcing[n] = source[...] + jnp.where(row_id == 0, values[:, None, :], 0.0)

    step = window // 2 if window % 16 == 0 else window
    lane = lax.broadcasted_iota(jnp.int32, (step, cols), 1)
    line = lax.broadcasted_iota(jnp.int32, (step, cols), 0)
    pieces = []
    for i in range(planes):
        p = jnp.where(odd == 1, planes - 1 - i, i)
        pieces += [(i, p, r) for r in range(0, window, step)]

    def neighbours(read, p, r):
        core = read(p + 1, r)
        if r > 0:
            above = read(p + 1, r - 1)
        else:
            above = jnp.where(line == 0, 0.0, pltpu.roll(core, 1, 0))
        if r + step < window:
            below = read(p + 1, r + 1)
        else:
            below = jnp.where(line == step - 1, 0.0, pltpu.roll(core, step - 1, 0))
        left = jnp.where(lane == 0, 0.0, pltpu.roll(core, 1, 1))
        right = jnp.where(lane == cols - 1, 0.0, pltpu.roll(core, cols - 1, 1))
        return core, read(p, r) + read(p + 2, r) + above + below + left + right

    def reader(key):
        return lambda p, r: field[slots[key], p, pl.ds(r, step)]

    def difference(new, old):
        return lambda p, r: field[slots[new], p, pl.ds(r, step)] - field[slots[old], p, pl.ds(r, step)]

    def piece(ref, p, r):
        return ref[p, pl.ds(r, step)]

    def result(n, end):
        def remote(target, source_slice):
            return pltpu.make_async_remote_copy(
                src_ref=field.at[slots[end], inner, pl.ds(own_at, own_rows)],
                dst_ref=out_hbm.at[0, :, pl.ds(pl.multiple_of(source_slice * own_rows, 8), own_rows)],
                send_sem=out_send.at[target],
                recv_sem=out_recv.at[source_slice],
                device_id={"tm": target},
            )
        return remote

    def own_copy(n):
        return pltpu.make_async_copy(
            field.at[slots[ends[n]], inner, pl.ds(own_at, own_rows)],
            out_hbm.at[0, :, pl.ds(n * own_rows, own_rows)],
            own_sem.at[1],
        )

    def emit(key):
        for n, end in enumerate(ends):
            if end == key:

                @pl.when(t != n)
                def _():
                    result(n, end)(n, t).start()

                @pl.when(t == n)
                def _():
                    own_copy(n).start()

    for tasks in rounds:
        for task in tasks:
            if task[0] == "coarse":
                _, n, source_key, target = task
                arrive(source_key)
                for i, p, r in pieces:
                    core, around = neighbours(reader(source_key), p, r)
                    field[slots[target], p + 1, pl.ds(r, step)] = core + piece(scale, p, r) * (
                        around - 6.0 * core + piece(forcing.at[n], p, r)
                    )
                    if i == 0 and r + step == window:
                        send(target, (0,))
            else:
                _, n, source_key, target, j, pair = task
                held = source_key[0] % 2 * slices + n
                arrive(source_key)
                if pair is not None:
                    arrive(pair[0])
                    arrive(pair[1])
                for i, p, r in pieces:
                    core, around = neighbours(reader(source_key), p, r)
                    gain = piece(inv, p, r)
                    if j == 1:
                        constant = core - gain * (6.0 * step_fine * core - step_fine * piece(forcing.at[n], p, r))
                        base[held, p, pl.ds(r, step)] = constant
                    else:
                        constant = piece(base.at[held], p, r)
                    value = constant + step_fine * gain * around
                    if pair is not None:
                        change, spread = neighbours(difference(*pair), p, r)
                        value = value + change + piece(scale, p, r) * (spread - 6.0 * change)
                    field[slots[target], p + 1, pl.ds(r, step)] = value
                    if i == 0 and r + step == window:
                        send(target, (0,))
            send(target, (1,))
            emit(target)

    for key in sorted(sent):
        arrive(key)
        for side, there in ((0, low_there), (1, high_there)):

            @pl.when(there)
            def _():
                halo(key, side).wait_send()

    for copy in ctrl_copies:
        copy.wait_send()
    for n in range(slices):

        @pl.when(t != n)
        def _():
            result(n, ends[n])(n, t).wait_send()
            result(n, ends[n])(t, n).wait_recv()

        @pl.when(t == n)
        def _():
            own_copy(n).wait()


def solution(mesh):
    slices, count = mesh.shape["tm"], mesh.shape["space"]
    plan = make_plan(slices)

    def on_device(initial_state, capacity, source, control, segment_index):
        planes, rows, cols = initial_state.shape
        own_rows = rows // slices
        reach = -(-(CORRECTIONS * SWEEPS + slices - CORRECTIONS) // 8) * 8
        window = min(rows, own_rows + 2 * reach)
        fields = len(plan[0])
        size = (planes, window, own_rows, reach, rows, cols, slices, count)
        block = (planes, window, cols)
        dma = pltpu.SemaphoreType.DMA
        return pl.pallas_call(
            functools.partial(kernel, plan, size),
            out_shape=jax.ShapeDtypeStruct((1, planes, rows, cols), jnp.float32),
            in_specs=[pl.BlockSpec(memory_space=pl.ANY)] * 3 + [pl.BlockSpec(memory_space=pltpu.VMEM)] * 2,
            out_specs=pl.BlockSpec(memory_space=pl.ANY),
            scratch_shapes=[
                pltpu.VMEM((fields, planes + 2, window, cols), jnp.float32),
                pltpu.VMEM((slices,) + block, jnp.float32),
                pltpu.VMEM((2 * slices,) + block, jnp.float32),
                pltpu.VMEM(block, jnp.float32),
                pltpu.VMEM(block, jnp.float32),
                pltpu.VMEM(block, jnp.float32),
                pltpu.VMEM((slices,) + control.shape, jnp.float32),
                dma((fields, 2)),
                dma((fields, 2)),
                dma((3,)),
                dma((slices,)),
                dma((slices,)),
                dma((slices,)),
                dma((slices,)),
                dma((2,)),
            ],
            compiler_params=pltpu.CompilerParams(
                collective_id=0, has_side_effects=True, vmem_limit_bytes=67043328 - 1048576
            ),
        )(initial_state, capacity, source, control, segment_index)

    return jax.shard_map(
        on_device,
        mesh=mesh,
        in_specs=(
            P("space", None, None),
            P("space", None, None),
            P("space", None, None),
            P("tm", None),
            P("space", None),
        ),
        out_specs=P("tm", "space", None, None),
        check_vma=False,
    )
```
